32 devices in a mesh: groups: 2 (over y), ctx: 4 (over z), head: 2 (over x), rep: 2 (over core).
Axes of the slice: x: 2, y: 2, z: 4, core: 2. Of those that a mesh axis runs over, the one named last changes fastest.
Arguments:
- kv_cache: bfloat16 [4, 96, 128, 576], P(('groups', 'rep'), 'ctx'), parts along dimension 0, may hold values from -10 to 10
- queries: bfloat16 [4, 4, 128, 576], P(('groups', 'rep'), None, 'head'), parts along dimension 0, may hold values from -45 to 45
- new_latent: bfloat16 [4, 4, 576], P(('groups', 'rep')), parts along dimension 0, may hold values from -6 to 6
- page_counts: int32 [4, 4], P(('groups', 'rep')), parts along dimension 0, may hold values from 1 to 36, 72 in all within a row
- page_tails: int32 [4, 4], P(('groups', 'rep')), parts along dimension 0, may hold values from 1 to 128
- page_slots: int32 [4, 96], P(('groups', 'rep')), parts along dimension 0, may hold values from 0 to 95, each once within a row
Outputs:
- attended: bfloat16 [4, 4, 128, 512], P(('groups', 'rep'), None, 'head'), parts along dimension 0
The draws below stay inside these ranges and needn't reach their ends.
There are 2 independent parts, one for each index of `groups`. The reference program is written for one: setup_inputs(seed, part) draws one part's arguments, and reference() takes and returns one part's arrays. A program takes and returns all parts, laid end to end along the dimension named above; each array names one. Nothing has to cross between parts.
Inputs may be any that keep to these rules, and one draw needn't show every extreme that they name: `page_counts`: the 4 counts of a half sum to 72, and the largest is exactly 36. `page_slots`: each half's row holds every slot once; only its first 72 entries are pages in use.
All inputs are finite; a program needn't handle non-finite values.
Results may differ from the reference program's by a relative error of at most 0.0033.
Values sent between devices are 32-bit elements; how exact they have to be, the bound alone decides.
A program may use at most 64 MiB of HBM per device.

```python
import math
import jax
import jax.numpy as jnp
import numpy as np
from jax import lax

HEADS = 128
LATENT = 512
PAGE = 128
BATCH = 4
KVW = 576
CTX_SLOTS = 96
TOTAL_PAGES = 72
MAXPAGES = 36
N_REP = 2


def draw_kv_cache(key, part):
    base = jnp.clip(jax.random.normal(jax.random.fold_in(key, 3), (N_REP, CTX_SLOTS, PAGE, KVW), jnp.float32), -6.0, 6.0)
    return base.astype(jnp.bfloat16)


def draw_queries(key, part):
    base = jnp.clip(jax.random.normal(jax.random.fold_in(key, 7), (N_REP, BATCH, HEADS, KVW), jnp.float32), -6.0, 6.0)
    return base.astype(jnp.bfloat16)


def plant(values, stream_key, low, largest):
    dims = values.shape
    place = [jax.random.randint(jax.random.fold_in(stream_key, axis), (), 0, dims[axis]) for axis in range(len(dims))]
    values = values.at[tuple(place)].set(low)
    longest = dims.index(max(dims))
    place[longest] = (place[longest] + 1) % dims[longest]
    return values.at[tuple(place)].set(largest)


def block_levels(own_key, shape, shards, low, high):
    def one(axis_at, shards_of):
        steps = jax.random.uniform(jax.random.fold_in(jax.random.fold_in(own_key, 6), axis_at), (shards_of,), jnp.float32, low / len(shards), high / len(shards))
        return jnp.repeat(jnp.exp(steps), shape[axis_at] // shards_of).reshape((-1,) + (1,) * (len(shape) - axis_at - 1))

    loudness = one(*shards[0])
    for cut in shards[1:]:
        loudness = loudness * one(*cut)
    return loudness


def length_profile(number_of, total, limit, skew):
    portions = [(1 << 20) // math.isqrt(rank ** skew) + 1 for rank in range(2, number_of + 1)]
    spare, given = total - limit - (number_of - 1), [1] * (number_of - 1)
    while spare > 0:
        movable = [i for i in range(number_of - 1) if given[i] < limit]
        whole, left = sum([portions[i] for i in movable]), spare
        for i in movable:
            more = min(limit - given[i], max(1, left * portions[i] // whole), spare)
            given[i] = given[i] + more
            spare = spare - more
    return np.array([limit] + given)


def ragged_sizes(key, count, total, reach, lean):
    if count == 2:
        one = jax.random.randint(key, (), max(1, total - reach), min(reach, total - 1) + 1)
        return jnp.stack([one, total - one])
    sizes = jnp.asarray(length_profile(count, total, reach, lean), jnp.int32)
    twos = (count - 1) // 2
    source_of, taker = sizes[1:1 + 2 * twos:2], sizes[2:2 + 2 * twos:2]
    margin = jnp.minimum(source_of - 1, reach - taker)
    moved = jax.random.randint(jax.random.fold_in(key, 1), (twos,), 0, 1 << 20) % (margin + 1)
    sizes = sizes.at[1:1 + 2 * twos:2].set(source_of - moved).at[2:2 + 2 * twos:2].set(taker + moved)
    return sizes[jax.random.permutation(jax.random.fold_in(key, 2), count)]


def gaussian(own_key, extent, width, limit, pieces=(), kind=jnp.bfloat16):
    level = block_levels(own_key, extent, pieces, -0.22, 0.18) if pieces else 1.0
    values = jax.random.normal(own_key, extent, jnp.float32) * width * level
    return jnp.minimum(jnp.maximum(values, -limit), limit).astype(kind)


def setup_inputs(seed: int = 0, part: int = 0) -> dict:
    key_list = jax.random.split(jax.random.key(seed), 7)
    part_keys = jax.random.split(jax.random.fold_in(key_list[6], part), 7)
    return {
        "kv_cache": draw_kv_cache(jax.random.fold_in(jax.random.fold_in(key_list[6], part), 71), part),
        "queries": draw_queries(jax.random.fold_in(jax.random.fold_in(key_list[6], part), 71), part),
        "new_latent": gaussian(part_keys[2], (N_REP, BATCH, KVW), 1.0, 6.0, ((0, 2),)),
        "page_counts": jax.vmap(lambda own: ragged_sizes(own, BATCH, TOTAL_PAGES, MAXPAGES, 2))(jax.random.split(part_keys[3], N_REP)).reshape((N_REP, BATCH)).astype(jnp.int32),
        "page_tails": plant(jax.random.randint(part_keys[4], (N_REP, BATCH), 1, PAGE + 1), jax.random.fold_in(part_keys[4], 1), 1, PAGE).astype(jnp.int32),
        "page_slots": jax.vmap(lambda own: jax.random.permutation(own, CTX_SLOTS))(jax.random.split(part_keys[5], N_REP)).reshape((N_REP, CTX_SLOTS)).astype(jnp.int32),
    }


score_scale = 192.0 ** -0.5
neg_large = -1.0e30


def page_partials(query_pages, cache_pages, token_valid):
    scores = jnp.einsum("phc,ptc->pht", query_pages.astype(jnp.float32), cache_pages.astype(jnp.float32)) * score_scale
    masked = jnp.where(token_valid[:, None, :], scores, neg_large)
    page_max = jnp.max(masked, axis=2)
    weights = jnp.where(token_valid[:, None, :], jnp.exp(masked - page_max[:, :, None]), 0.0).astype(jnp.bfloat16)
    page_sum = jnp.sum(weights.astype(jnp.float32), axis=2)
    page_acc = jnp.einsum("pht,ptc->phc", weights.astype(jnp.float32), cache_pages[:, :, :LATENT].astype(jnp.float32))
    return page_max, page_sum, page_acc


def reference(kv_cache, queries, new_latent, page_counts, page_tails, page_slots):
    halves = []
    for half in range(N_REP):
        counts = page_counts[half]
        ends = jnp.cumsum(counts).astype(jnp.int32)
        starts = (ends - counts).astype(jnp.int32)
        lengths = ((counts - 1) * PAGE + page_tails[half]).astype(jnp.int32)
        cache_half = kv_cache[half]
        slots_half = page_slots[half]

        def one_sequence(index):
            page_index = jnp.arange(MAXPAGES, dtype=jnp.int32)
            page_ok = page_index < jnp.take(counts, index)
            ranks = jnp.clip(jnp.take(starts, index) + page_index, 0, CTX_SLOTS - 1).astype(jnp.int32)
            slots = jnp.take(slots_half, ranks).astype(jnp.int32)
            cache_pages = jnp.take(cache_half, slots, axis=0)
            token_place = page_index[:, None] * PAGE + jnp.arange(PAGE, dtype=jnp.int32)[None, :]
            token_valid = page_ok[:, None] & (token_place < jnp.take(lengths, index))
            query_rows = queries[half][index]
            query_pages = jnp.broadcast_to(query_rows[None], (MAXPAGES,) + query_rows.shape)
            page_max, page_sum, page_acc = page_partials(query_pages, cache_pages, token_valid)
            own_row = new_latent[half][index].astype(jnp.float32)
            own_score = jnp.sum(query_rows.astype(jnp.float32) * own_row[None, :], axis=1) * score_scale
            top = jnp.maximum(jnp.max(page_max, axis=0), own_score)
            factor = jnp.exp(page_max - top[None, :])
            own_factor = jnp.exp(own_score - top)
            numer = jnp.sum(factor[:, :, None] * page_acc, axis=0) + own_factor[:, None] * own_row[None, :LATENT]
            denom = jnp.sum(factor * page_sum, axis=0) + own_factor
            return (numer / denom[:, None]).astype(jnp.bfloat16)

        halves.append(lax.map(one_sequence, jnp.arange(BATCH, dtype=jnp.int32)))
    return jnp.stack(halves)
```

```python
import functools
import math

import jax
import jax.numpy as jnp
from jax import lax
from jax.experimental import pallas as pl
from jax.experimental.pallas import tpu as pltpu
from jax.sharding import PartitionSpec as P

LATENT = 512
SCALE = 192.0 ** (-0.5) * math.log2(math.e)
NEG = -1e30
KV_COPIES = 6
PIECES = 2
LAG = 2
MESH = pl.DeviceIdType.MESH


def kernel(
    n,
    counts_ref,
    tails_ref,
    slots_ref,
    latent_ref,
    q_hbm,
    kv_hbm,
    out_ref,
    q_v,
    kv_v,
    bias_v,
    score_v,
    weight_v,
    acc_v,
    inbox,
    part_v,
    cross,
    total_v,
    final,
    stat_out,
    stat_in,
    load_sem,
    stat_send,
    stat_recv,
    in_send,
    in_recv,
    cross_recv,
    fin_send,
    fin_recv,
):
    batch, rows, width = q_v.shape
    pages, page, _ = kv_hbm.shape[1:]
    tokens = pages * page
    slots = slots_ref.shape[1]
    me = lax.axis_index("ctx")
    half = n // 2
    left = me < half
    inward = jnp.where(left, me + 1, me - 1)
    outward = jnp.where(left, me - 1, me + 1)
    is_end = (me == 0) | (me == n - 1)
    is_mid = (me == half - 1) | (me == half)
    inner = jnp.logical_not(is_end)

    loads = [pltpu.make_async_copy(q_hbm.at[0], q_v, load_sem.at[KV_COPIES])]
    step = pages // KV_COPIES
    for i in range(KV_COPIES):
        loads.append(
            pltpu.make_async_copy(
                kv_hbm.at[0, pl.ds(i * step, step)],
                kv_v.at[pl.ds(i * step, step)],
                load_sem.at[i],
            )
        )
    for load in loads:
        load.start()

    barrier = pltpu.get_barrier_semaphore()

    @pl.loop(1, n)
    def _(off):
        pl.semaphore_signal(
            barrier, inc=1, device_id={"ctx": lax.rem(me + off, n)}, device_id_type=MESH
        )

    kv_v[pages] = jnp.zeros((page, width), jnp.bfloat16)
    kv_v[pages, 0:batch, :] = latent_ref[0]

    slot_id = me * pages + lax.broadcasted_iota(jnp.int32, (pages, slots), 0)
    rank = lax.broadcasted_iota(jnp.int32, (pages, slots), 1)
    match = slots_ref[...] == slot_id
    lane = lax.broadcasted_iota(jnp.int32, (pages, page), 1)
    lane_own = lax.broadcasted_iota(jnp.int32, (8, page), 1)
    begin = jnp.int32(0)
    for s in range(batch):
        count = counts_ref[0, s]
        length = (count - 1) * page + tails_ref[0, s]
        place = rank - begin
        inside = match & (place >= 0) & (place < count)
        limit = jnp.sum(
            jnp.where(inside, (length - place * page).astype(jnp.float32), 0.0),
            axis=1,
            keepdims=True,
        )
        bias_v[s, 0:pages, :] = jnp.where(lane.astype(jnp.float32) < limit, 0.0, NEG)
        own_here = (lane_own == s) & (me == 0)
        bias_v[s, pages : pages + 8, :] = jnp.where(own_here, 0.0, NEG)
        begin = begin + count

    loads[0].wait()
    queries = q_v[...].reshape(batch * rows, width)
    tops = [jnp.full((rows, page), NEG, jnp.float32) for _ in range(batch)]
    nt = (((1,), (1,)), ((), ()))
    for first in range(0, pages + 1, 2):
        if first < pages and first % step == 0:
            loads[1 + first // step].wait()
        many = min(2, pages + 1 - first)
        keys = kv_v[first : first + many].reshape(many * page, width)
        block = lax.dot_general(queries, keys, nt, preferred_element_type=jnp.float32)
        for s in range(batch):
            for j in range(many):
                at = first + j
                value = (
                    block[s * rows : (s + 1) * rows, j * page : (j + 1) * page] * SCALE
                    + bias_v[s, at : at + 1, :]
                )
                score_v[s, :, at * page : (at + 1) * page] = value
                tops[s] = jnp.maximum(tops[s], value)

    size = rows // PIECES

    def piece(k):
        return k // PIECES, pl.ds((k % PIECES) * size, size)

    def ship(source, target, send, recv, k, to):
        s, at = piece(k)
        return pltpu.make_async_remote_copy(
            src_ref=source.at[s, at],
            dst_ref=target.at[s, at],
            send_sem=send.at[k],
            recv_sem=recv.at[k],
            device_id={"ctx": to},
            device_id_type=MESH,
        )

    def stat_copy(s, to, origin, slot):
        return pltpu.make_async_remote_copy(
            src_ref=stat_out.at[s],
            dst_ref=stat_in.at[s, origin],
            send_sem=stat_send.at[s, slot],
            recv_sem=stat_recv.at[s, origin],
            device_id={"ctx": to},
            device_id_type=MESH,
        )

    def other(off):
        to = lax.rem(me + off, n)
        return to, (to > 0) & (to < n - 1)

    lane_row = lax.broadcasted_iota(jnp.int32, (rows, page), 1)
    for s in range(batch):
        top = jnp.max(tops[s], axis=1, keepdims=True)
        total = jnp.zeros((rows, page), jnp.float32)
        for at in range(pages + 1):
            cols = slice(at * page, (at + 1) * page)
            weight = jnp.exp2(score_v[s, :, cols] - top).astype(jnp.bfloat16)
            weight_v[s % 2, :, cols] = weight
            total = total + weight.astype(jnp.float32)
        total = jnp.sum(total, axis=1, keepdims=True)
        pair = jnp.where(lane_row == 0, top, total)
        square = jnp.concatenate([pair] * (page // rows), axis=0)
        tile = jnp.transpose(square)[0:8]
        stat_out[s] = tile
        stat_in[s, pl.ds(me, 1)] = tile[None]
        if s == 0:
            pl.semaphore_wait(barrier, n - 1)

        @pl.loop(1, n)
        def _(off):
            to, wanted = other(off)

            @pl.when(wanted)
            def _():
                stat_copy(s, to, me, off).start()

        values = kv_v[...].reshape(tokens + page, width)[:, :LATENT]
        acc_v[s] = jnp.dot(weight_v[s % 2], values, preferred_element_type=jnp.float32)

        @pl.when(is_end)
        def _():
            for k in range(s * PIECES, (s + 1) * PIECES):
                ship(acc_v, inbox, in_send, in_recv, k, inward).start()

    number = batch * PIECES
    from_end = (outward == 0) | (outward == n - 1)

    def factors(s):
        @pl.loop(1, n)
        def _(off):
            stat_copy(s, me, lax.rem(me + off, n), off).wait_recv()

        best = stat_in[s, 0]
        for j in range(1, n):
            best = jnp.maximum(best, stat_in[s, j])
        best = best[0:1]
        denom = jnp.zeros((1, page), jnp.float32)
        mine = jnp.zeros((1, page), jnp.float32)
        theirs = jnp.zeros((1, page), jnp.float32)
        for j in range(n):
            tile = stat_in[s, j]
            keep = jnp.exp2(tile[0:1] - best)
            denom = denom + keep * tile[1:2]
            mine = jnp.where(me == j, keep, mine)
            theirs = jnp.where(outward == j, keep, theirs)
        mine = mine / denom
        theirs = jnp.where(from_end, theirs / denom, 1.0)
        row = lax.broadcasted_iota(jnp.int32, (page, page), 0)
        turned = jnp.transpose(jnp.where(row == 0, mine, theirs))
        return turned[0:rows, 0:1], turned[0:rows, 1:2]

    @pl.when(inner)
    def _():
        scales = {}
        for k in range(number + LAG):
            if k < number:
                s, at = piece(k)
                if k % PIECES == 0:
                    scales[s] = factors(s)
                lo = (k % PIECES) * size
                mine, theirs = (f[lo : lo + size] for f in scales[s])
                ship(acc_v, inbox, in_send, in_recv, k, inward).wait_recv()
                part_v[s, at] = acc_v[s, at] * mine + inbox[s, at] * theirs

                @pl.when(is_mid)
                def _():
                    ship(part_v, cross, in_send, cross_recv, k, inward).start()

                @pl.when(jnp.logical_not(is_mid))
                def _():
                    ship(part_v, inbox, in_send, in_recv, k, inward).start()

            if k >= LAG:
                d = k - LAG
                s, at = piece(d)

                @pl.when(is_mid)
                def _():
                    ship(part_v, cross, in_send, cross_recv, d, inward).wait_recv()
                    total = part_v[s, at] + cross[s, at]
                    total_v[s, at] = total
                    ship(total_v, final, fin_send, fin_recv, d, outward).start()
                    out_ref[0, s, at] = total.astype(jnp.bfloat16)

                @pl.when(jnp.logical_not(is_mid))
                def _():
                    ship(final, final, fin_send, fin_recv, d, outward).wait_recv()
                    ship(final, final, fin_send, fin_recv, d, outward).start()
                    out_ref[0, s, at] = final[s, at].astype(jnp.bfloat16)

        for k in range(number):
            ship(total_v, final, fin_send, fin_recv, k, outward).wait_send()

    @pl.when(is_end)
    def _():
        for k in range(number):
            s, at = piece(k)
            ship(total_v, final, fin_send, fin_recv, k, inward).wait_recv()
            out_ref[0, s, at] = final[s, at].astype(jnp.bfloat16)

    for k in range(number):
        ship(part_v, inbox, in_send, in_recv, k, inward).wait_send()
    for s in range(batch):

        @pl.loop(1, n)
        def _(off):
            to, wanted = other(off)

            @pl.when(wanted)
            def _():
                stat_copy(s, to, me, off).wait_send()


def local(n, kv_cache, queries, new_latent, page_counts, page_tails, page_slots):
    _, pages, page, width = kv_cache.shape
    _, batch, rows, _ = queries.shape
    number = batch * PIECES
    block = (batch, rows, LATENT)
    vmem = pl.BlockSpec(memory_space=pltpu.VMEM)
    smem = pl.BlockSpec(memory_space=pltpu.SMEM)
    hbm = pl.BlockSpec(memory_space=pl.ANY)
    dma = pltpu.SemaphoreType.DMA
    return pl.pallas_call(
        functools.partial(kernel, n),
        out_shape=jax.ShapeDtypeStruct((1,) + block, jnp.bfloat16),
        in_specs=[smem, smem, vmem, vmem, hbm, hbm],
        out_specs=vmem,
        scratch_shapes=[
            pltpu.VMEM((batch, rows, width), jnp.bfloat16),
            pltpu.VMEM((pages + 1, page, width), jnp.bfloat16),
            pltpu.VMEM((batch, pages + 8, page), jnp.float32),
            pltpu.VMEM((batch, rows, (pages + 1) * page), jnp.float32),
            pltpu.VMEM((2, rows, (pages + 1) * page), jnp.bfloat16),
            pltpu.VMEM(block, jnp.float32),
            pltpu.VMEM(block, jnp.float32),
            pltpu.VMEM(block, jnp.float32),
            pltpu.VMEM(block, jnp.float32),
            pltpu.VMEM(block, jnp.float32),
            pltpu.VMEM(block, jnp.float32),
            pltpu.VMEM((batch, 8, page), jnp.float32),
            pltpu.VMEM((batch, n, 8, page), jnp.float32),
            dma((KV_COPIES + 1,)),
            dma((batch, n)),
            dma((batch, n)),
            dma((number,)),
            dma((number,)),
            dma((number,)),
            dma((number,)),
            dma((number,)),
        ],
        compiler_params=pltpu.CompilerParams(collective_id=0, has_side_effects=True),
    )(page_counts, page_tails, page_slots, new_latent, queries, kv_cache)


def solution(mesh):
    in_specs = (
        P(("groups", "rep"), "ctx", None, None),
        P(("groups", "rep"), None, "head", None),
        P(("groups", "rep"), None, None),
        P(("groups", "rep"), None),
        P(("groups", "rep"), None),
        P(("groups", "rep"), None),
    )
    out_specs = P(("groups", "rep"), None, "head", None)
    return jax.shard_map(
        functools.partial(local, mesh.shape["ctx"]),
        mesh=mesh,
        in_specs=in_specs,
        out_specs=out_specs,
        check_vma=False,
    )
```

```python
import functools
import math

import jax
import jax.numpy as jnp
from jax import lax
from jax.experimental import pallas as pl
from jax.experimental.pallas import tpu as pltpu
from jax.sharding import PartitionSpec as P

LATENT = 512
SCALE = 192.0 ** (-0.5) * math.log2(math.e)
NEG = -1e30
PIECES = 4
LAG = 6
MESH = pl.DeviceIdType.MESH


def kernel(
    n,
    counts_ref,
    tails_ref,
    slots_ref,
    latent_ref,
    q_hbm,
    kv_hbm,
    out_ref,
    q_v,
    kv_v,
    own_v,
    bias_v,
    score_v,
    weight_v,
    acc_v,
    inbox,
    part_v,
    cross,
    total_v,
    final,
    stat_out,
    stat_in,
    load_sem,
    stat_send,
    stat_recv,
    in_send,
    in_recv,
    cross_recv,
    fin_send,
    fin_recv,
):
    batch, rows, width = q_v.shape
    pages, _, page = kv_hbm.shape[1:]
    tokens = pages * page
    slots = slots_ref.shape[1]
    me = lax.axis_index("ctx")
    half = n // 2
    left = me < half
    inward = jnp.where(left, me + 1, me - 1)
    outward = jnp.where(left, me - 1, me + 1)
    is_end = (me == 0) | (me == n - 1)
    is_mid = (me == half - 1) | (me == half)
    inner = jnp.logical_not(is_end)

    loads = [pltpu.make_async_copy(q_hbm.at[0], q_v, load_sem.at[pages])]
    for i in range(pages):
        loads.append(
            pltpu.make_async_copy(
                kv_hbm.at[0, i],
                kv_v.at[:, pl.ds(i * page, page)],
                load_sem.at[i],
            )
        )
    for load in loads:
        load.start()

    barrier = pltpu.get_barrier_semaphore()

    @pl.loop(1, n)
    def _(off):
        pl.semaphore_signal(
            barrier, inc=1, device_id={"ctx": lax.rem(me + off, n)}, device_id_type=MESH
        )

    own_v[...] = jnp.zeros((page, width), jnp.bfloat16)
    own_v[0:batch, :] = latent_ref[0]

    slot_id = me * pages + lax.broadcasted_iota(jnp.int32, (pages, slots), 0)
    rank = lax.broadcasted_iota(jnp.int32, (pages, slots), 1)
    match = slots_ref[...] == slot_id
    lane = lax.broadcasted_iota(jnp.int32, (pages, page), 1)
    lane_own = lax.broadcasted_iota(jnp.int32, (8, page), 1)
    begin = jnp.int32(0)
    for s in range(batch):
        count = counts_ref[0, s]
        length = (count - 1) * page + tails_ref[0, s]
        place = rank - begin
        inside = match & (place >= 0) & (place < count)
        limit = jnp.sum(
            jnp.where(inside, (length - place * page).astype(jnp.float32), 0.0),
            axis=1,
            keepdims=True,
        )
        bias_v[s, 0:pages, :] = jnp.where(lane.astype(jnp.float32) < limit, 0.0, NEG)
        own_here = (lane_own == s) & (me == 0)
        bias_v[s, pages : pages + 8, :] = jnp.where(own_here, 0.0, NEG)
        begin = begin + count

    loads[0].wait()
    queries = q_v[...].reshape(batch * rows, width)
    tops = [jnp.full((rows, page), NEG, jnp.float32) for _ in range(batch)]
    nt = (((1,), (1,)), ((), ()))
    for first in [*range(0, pages, 2), pages]:
        many = min(2, pages - first) or 1
        if first < pages:
            for j in range(many):
                loads[1 + first + j].wait()
            keys = kv_v[:, first * page : (first + many) * page]
            block = jnp.dot(queries, keys, preferred_element_type=jnp.float32)
        else:
            block = lax.dot_general(
                queries, own_v[...], nt, preferred_element_type=jnp.float32
            )
        for s in range(batch):
            for j in range(many):
                at = first + j
                value = (
                    block[s * rows : (s + 1) * rows, j * page : (j + 1) * page] * SCALE
                    + bias_v[s, at : at + 1, :]
                )
                score_v[s, :, at * page : (at + 1) * page] = value
                tops[s] = jnp.maximum(tops[s], value)

    size = batch * rows // PIECES
    wide = out_ref.shape[3] // page

    def piece(k):
        return k // PIECES, pl.ds((k % PIECES) * size, size)

    def ship(source, target, send, recv, k, to):
        s, at = piece(k)
        return pltpu.make_async_remote_copy(
            src_ref=source.at[s, at],
            dst_ref=target.at[s, at],
            send_sem=send.at[k],
            recv_sem=recv.at[k],
            device_id={"ctx": to},
            device_id_type=MESH,
        )

    def stat_copy(s, to, origin, slot):
        return pltpu.make_async_remote_copy(
            src_ref=stat_out.at[s],
            dst_ref=stat_in.at[s, origin],
            send_sem=stat_send.at[s, slot],
            recv_sem=stat_recv.at[s, origin],
            device_id={"ctx": to},
            device_id_type=MESH,
        )

    def other(off):
        to = lax.rem(me + off, n)
        return to, (to > 0) & (to < n - 1)

    lane_row = lax.broadcasted_iota(jnp.int32, (rows, page), 1)
    for s in range(batch):
        top = jnp.max(tops[s], axis=1, keepdims=True)
        total = jnp.zeros((rows, page), jnp.float32)
        for at in range(pages + 1):
            cols = slice(at * page, (at + 1) * page)
            weight = jnp.exp2(score_v[s, :, cols] - top).astype(jnp.bfloat16)
            weight_v[s * rows : (s + 1) * rows, cols] = weight
            total = total + weight.astype(jnp.float32)
        total = jnp.sum(total, axis=1, keepdims=True)
        pair = jnp.where(lane_row == 0, top, total)
        square = jnp.concatenate([pair] * (page // rows), axis=0)
        tile = jnp.transpose(square)[0:8]
        stat_out[s] = tile
        stat_in[s, pl.ds(me, 1)] = tile[None]
        if s == 0:
            pl.semaphore_wait(barrier, n - 1)

        @pl.loop(1, n)
        def _(off):
            to, wanted = other(off)

            @pl.when(wanted)
            def _():
                stat_copy(s, to, me, off).start()

    group = 2
    for j in range(0, wide, group):
        span = slice(j * page, (j + group) * page)
        block = lax.dot_general(
            weight_v[:, 0:tokens], kv_v[span, :], nt, preferred_element_type=jnp.float32
        ) + jnp.dot(
            weight_v[:, tokens:], own_v[:, span], preferred_element_type=jnp.float32
        )
        for i in range(group):
            acc_v[j + i] = block[:, i * page : (i + 1) * page]

        @pl.when(is_end)
        def _():
            for k in range(j * PIECES, (j + group) * PIECES):
                ship(acc_v, inbox, in_send, in_recv, k, inward).start()

    def emit(k, value):
        j = k // PIECES
        first = (k % PIECES) * size
        value = value.astype(jnp.bfloat16)
        for lo in range(0, size, min(size, rows)):
            s, r = divmod(first + lo, rows)
            out_ref[0, s, r : r + min(size, rows), j * page : (j + 1) * page] = value[
                lo : lo + min(size, rows)
            ]

    number = wide * PIECES
    from_end = (outward == 0) | (outward == n - 1)

    def factors(s):
        @pl.loop(1, n)
        def _(off):
            stat_copy(s, me, lax.rem(me + off, n), off).wait_recv()

        best = stat_in[s, 0]
        for j in range(1, n):
            best = jnp.maximum(best, stat_in[s, j])
        best = best[0:1]
        denom = jnp.zeros((1, page), jnp.float32)
        mine = jnp.zeros((1, page), jnp.float32)
        theirs = jnp.zeros((1, page), jnp.float32)
        for j in range(n):
            tile = stat_in[s, j]
            keep = jnp.exp2(tile[0:1] - best)
            denom = denom + keep * tile[1:2]
            mine = jnp.where(me == j, keep, mine)
            theirs = jnp.where(outward == j, keep, theirs)
        mine = mine / denom
        theirs = jnp.where(from_end, theirs / denom, 1.0)
        row = lax.broadcasted_iota(jnp.int32, (page, page), 0)
        turned = jnp.transpose(jnp.where(row == 0, mine, theirs))
        return turned[0:rows, 0:1], turned[0:rows, 1:2]

    @pl.when(inner)
    def _():
        pairs = [factors(s) for s in range(batch)]
        scales = [jnp.concatenate(f, axis=0) for f in zip(*pairs)]
        for k in range(number + LAG):
            if k < number:
                s, at = piece(k)
                lo = (k % PIECES) * size
                mine, theirs = (f[lo : lo + size] for f in scales)
                ship(acc_v, inbox, in_send, in_recv, k, inward).wait_recv()
                part_v[s, at] = acc_v[s, at] * mine + inbox[s, at] * theirs

                @pl.when(is_mid)
                def _():
                    ship(part_v, cross, in_send, cross_recv, k, inward).start()

                @pl.when(jnp.logical_not(is_mid))
                def _():
                    ship(part_v, inbox, in_send, in_recv, k, inward).start()

            if k >= LAG:
                d = k - LAG
                s, at = piece(d)

                @pl.when(is_mid)
                def _():
                    ship(part_v, cross, in_send, cross_recv, d, inward).wait_recv()
                    total = part_v[s, at] + cross[s, at]
                    total_v[s, at] = total
                    ship(total_v, final, fin_send, fin_recv, d, outward).start()
                    emit(d, total)

                @pl.when(jnp.logical_not(is_mid))
                def _():
                    ship(final, final, fin_send, fin_recv, d, outward).wait_recv()
                    ship(final, final, fin_send, fin_recv, d, outward).start()
                    emit(d, final[s, at])

        for k in range(number):
            ship(total_v, final, fin_send, fin_recv, k, outward).wait_send()

    @pl.when(is_end)
    def _():
        for k in range(number):
            s, at = piece(k)
            ship(total_v, final, fin_send, fin_recv, k, inward).wait_recv()
            emit(k, final[s, at])

    for k in range(number):
        ship(part_v, inbox, in_send, in_recv, k, inward).wait_send()
    for s in range(batch):

        @pl.loop(1, n)
        def _(off):
            to, wanted = other(off)

            @pl.when(wanted)
            def _():
                stat_copy(s, to, me, off).wait_send()


def local(n, kv_cache, queries, new_latent, page_counts, page_tails, page_slots):
    _, pages, page, width = kv_cache.shape
    _, batch, rows, _ = queries.shape
    number = LATENT // page * PIECES
    block = (LATENT // page, batch * rows, page)
    vmem = pl.BlockSpec(memory_space=pltpu.VMEM)
    smem = pl.BlockSpec(memory_space=pltpu.SMEM)
    hbm = pl.BlockSpec(memory_space=pltpu.HBM)
    dma = pltpu.SemaphoreType.DMA
    return pl.pallas_call(
        functools.partial(kernel, n),
        out_shape=jax.ShapeDtypeStruct((1, batch, rows, LATENT), jnp.bfloat16),
        in_specs=[smem, smem, vmem, vmem, hbm, hbm],
        out_specs=vmem,
        scratch_shapes=[
            pltpu.VMEM((batch, rows, width), jnp.bfloat16),
            pltpu.VMEM((width, pages * page), jnp.bfloat16),
            pltpu.VMEM((page, width), jnp.bfloat16),
            pltpu.VMEM((batch, pages + 8, page), jnp.float32),
            pltpu.VMEM((batch, rows, (pages + 1) * page), jnp.float32),
            pltpu.VMEM((batch * rows, (pages + 1) * page), jnp.bfloat16),
            pltpu.VMEM(block, jnp.float32),
            pltpu.VMEM(block, jnp.float32),
            pltpu.VMEM(block, jnp.float32),
            pltpu.VMEM(block, jnp.float32),
            pltpu.VMEM(block, jnp.float32),
            pltpu.VMEM(block, jnp.float32),
            pltpu.VMEM((batch, 8, page), jnp.float32),
            pltpu.VMEM((batch, n, 8, page), jnp.float32),
            dma((pages + 1,)),
            dma((batch, n)),
            dma((batch, n)),
            dma((number,)),
            dma((number,)),
            dma((number,)),
            dma((number,)),
            dma((number,)),
        ],
        compiler_params=pltpu.CompilerParams(
            collective_id=0, has_side_effects=True
        ),
    )(page_counts, page_tails, page_slots, new_latent, queries, jnp.swapaxes(kv_cache, 2, 3))


def solution(mesh):
    in_specs = (
        P(("groups", "rep"), "ctx", None, None),
        P(("groups", "rep"), None, "head", None),
        P(("groups", "rep"), None, None),
        P(("groups", "rep"), None),
        P(("groups", "rep"), None),
        P(("groups", "rep"), None),
    )
    out_specs = P(("groups", "rep"), None, "head", None)
    return jax.shard_map(
        functools.partial(local, mesh.shape["ctx"]),
        mesh=mesh,
        in_specs=in_specs,
        out_specs=out_specs,
        check_vma=False,
    )
```
